32 devices in a mesh: row: 8 (over z, core), col: 4 (over y, x).
Axes of the slice: x: 2, y: 2, z: 4, core: 2. Of those that a mesh axis runs over, the one named last changes fastest.
Arguments:
- tokens: bfloat16 [512, 4096], P(None, 'col'), may hold values from -6 to 6
- w_gate: bfloat16 [4096, 10240], P('col', 'row'), may hold values from -0.09375 to 0.09375
- w_up: bfloat16 [4096, 10240], P('col', 'row'), may hold values from -0.09375 to 0.09375
- w_down: bfloat16 [10240, 4096], P('row', 'col'), may hold values from -0.0625 to 0.0625
Outputs:
- result: bfloat16 [512, 4096], P('row', 'col')
The draws below stay inside these ranges and needn't reach their ends.
All inputs are finite; a program needn't handle non-finite values.
Results may differ from the reference program's by a relative error of at most 0.025.
Values may be sent and summed in bfloat16 or wider, within the bound.
A program may use at most 64 MiB of HBM per device.

```python
import jax
import jax.numpy as jnp
from jax import lax

D = 4096
FF = 10240
TOKENS = 512
N_COL = 4


def block_levels(stream_key, extent, cuts, low, largest):
    def one(dim, shards_of):
        heights = jax.random.uniform(jax.random.fold_in(jax.random.fold_in(stream_key, 6), dim), (shards_of,), jnp.float32, low / len(cuts), largest / len(cuts))
        return jnp.repeat(jnp.exp(heights), extent[dim] // shards_of).reshape((-1,) + (1,) * (len(extent) - dim - 1))

    factor_of = one(*cuts[0])
    for cut in cuts[1:]:
        factor_of = factor_of * one(*cut)
    return factor_of


def gaussian(rng, dims, scale, reach, split=(), kind=jnp.bfloat16):
    gain = block_levels(rng, dims, split, -0.22, 0.18) if split else 1.0
    array = jax.random.normal(rng, dims, jnp.float32) * scale * gain
    return jnp.minimum(jnp.maximum(array, -reach), reach).astype(kind)


def setup_inputs(seed: int = 0) -> dict:
    key_of = jax.random.split(jax.random.key(seed), 5)
    return {
        "tokens": gaussian(key_of[0], (TOKENS, D), 1.0, 6.0, ((1, 4),)),
        "w_gate": gaussian(key_of[1], (D, FF), D ** -0.5, 0.09375, ((0, 4), (1, 8))),
        "w_up": gaussian(key_of[2], (D, FF), D ** -0.5, 0.09375, ((0, 4), (1, 8))),
        "w_down": gaussian(key_of[3], (FF, D), FF ** -0.5, 0.0625, ((0, 8), (1, 4))),
    }


def reference(tokens, w_gate, w_up, w_down):
    block_width = tokens.shape[1] // N_COL
    joined = jnp.concatenate([w_gate, w_up], axis=1)
    hidden_width = w_gate.shape[1]

    def accumulate(running, block_index):
        offset = (block_index * block_width).astype(jnp.int32)
        token_rows = lax.dynamic_slice_in_dim(tokens, offset, block_width, 1)
        weight_rows = lax.dynamic_slice_in_dim(joined, offset, block_width, 0)
        product = jnp.dot(token_rows, weight_rows, preferred_element_type=jnp.float32)
        rounded = lax.optimization_barrier(product.astype(jnp.bfloat16))
        return running + rounded.astype(jnp.float32), None

    initial = jnp.zeros((tokens.shape[0], 2 * hidden_width), jnp.float32)
    summed, _ = lax.scan(accumulate, initial, jnp.arange(N_COL, dtype=jnp.int32))
    pre_gate = summed[:, :hidden_width]
    pre_up = summed[:, hidden_width:]
    hidden = (jax.nn.gelu(pre_gate, approximate=True) * pre_up).astype(jnp.bfloat16)
    return jnp.dot(hidden, w_down, preferred_element_type=jnp.float32).astype(jnp.bfloat16)
```

```python
import functools

import jax
import jax.numpy as jnp
from jax import lax
from jax.experimental import pallas as pl
from jax.experimental.pallas import tpu as pltpu
from jax.sharding import PartitionSpec as P

MESH = pl.DeviceIdType.MESH
TILE = 256
SUBS = 2
AHEAD = 3


def activate(pre_gate, pre_up):
    return (jax.nn.gelu(pre_gate, approximate=True) * pre_up).astype(jnp.bfloat16)


def plain(tokens, w_gate, w_up, w_down):
    joined = jnp.concatenate([w_gate, w_up], axis=1)
    hidden_width = w_gate.shape[1]
    summed = lax.psum_scatter(
        jnp.dot(tokens, joined, preferred_element_type=jnp.float32).astype(jnp.bfloat16),
        "col",
        scatter_dimension=0,
        tiled=True,
    ).astype(jnp.float32)
    hidden = activate(summed[:, :hidden_width], summed[:, hidden_width:])
    hidden_all = lax.all_gather(hidden, "col", axis=0, tiled=True)
    result = lax.psum_scatter(
        jnp.dot(hidden_all, w_down, preferred_element_type=jnp.float32),
        "row",
        scatter_dimension=0,
        tiled=True,
    )
    return result.astype(jnp.bfloat16)


def schedule(chunks, ahead):
    late = {"s2": 0, "g1": 2, "s1": -ahead, "g2": 4, "c2": 7, "c1": 6}
    order = []
    for k in range(chunks + max(late.values())):
        for stage, lag in late.items():
            j = k - lag
            if 0 <= j < chunks and (stage != "s1" or j >= ahead):
                order.append((stage, j))
    return order


def kernel(
    n_row, tok_hbm, wg_hbm, wu_hbm, wd_hbm, out_ref,
    tok, w1, wd, s1, own, r1, s2, r2, hid, part, c1s, c1r, c2s, c2r,
    load_sem, send_sem, recv1, recv2, recv3, recv4, recv5, recv6,
):
    row, col = lax.axis_index("row"), lax.axis_index("col")
    y, x = col // 2, col % 2
    z, core = row // 2, row % 2
    n_z = n_row // 2
    chunks = s1.shape[0]
    remote_chunks = chunks - SUBS
    half = hid.shape[-1]
    x_peer = (row, 2 * y + 1 - x)
    y_peer = (row, 2 * (1 - y) + x)
    core_peer = (2 * z + 1 - core, col)
    upper = 2 * z // n_z

    def z_order(k):
        if k == n_z - 1:
            return z
        down = n_z - 1 - k - (z + k + 1) // n_z
        up = k + (k + n_z - z) // n_z
        return down * (1 - upper) + up * upper

    blocks = [z_order(k) for k in range(n_z)]
    z_peers = [(2 * other + core, col) for other in blocks[:-1]]
    first_peer, second_peer = (x_peer, y_peer), (y_peer, x_peer)
    first_at, second_at = (x, y), (y, x)

    barrier = pltpu.get_barrier_semaphore()
    peers = [x_peer, y_peer, core_peer] + z_peers
    for peer in peers:
        pl.semaphore_signal(barrier, inc=1, device_id=peer, device_id_type=MESH)

    def local(src, dst, sem):
        return pltpu.make_async_copy(src, dst, load_sem.at[sem])

    def load_tok(k):
        return local(tok_hbm.at[blocks[k]], tok.at[k], min(k, 1))

    def load_w1(m, k):
        w_hbm = (wg_hbm, wu_hbm)[k]
        return local(w_hbm.at[:, pl.ds(m * half, half)], w1.at[m, :, pl.ds(k * half, half)], 2 + 2 * m + k)

    load_wd = local(wd_hbm, wd, 6)
    load_tok(0).start()
    for k in range(2):
        load_w1(0, k).start()

    def remote(src, dst, send, recv, peer):
        return pltpu.make_async_remote_copy(
            src_ref=src, dst_ref=dst, send_sem=send_sem.at[send], recv_sem=recv, device_id=peer, device_id_type=MESH)

    def copy_s1(m, j):
        return remote(s1.at[j, m], r1.at[j, m], 0, recv1.at[j], first_peer[m])

    def copy_s2(m, j):
        return remote(s2.at[j, m], r2.at[j, m], 1, recv2.at[j], second_peer[m])

    def copy_g1(m, j):
        ref = hid.at[j, m, first_at[m], second_at[m]]
        return remote(ref, ref, 2, recv3.at[j], second_peer[m])

    def copy_g2(m, j):
        ref = hid.at[j, m, first_at[m]]
        return remote(ref, ref, 3, recv4.at[j], first_peer[m])

    def copy_c1(j):
        return remote(c1s.at[j], c1r.at[j], 4, recv5.at[j], core_peer)

    def copy_c2(j):
        k, sub = j // SUBS, j % SUBS
        slot = z - jnp.where(z > blocks[k], 1, 0)
        return remote(c2s.at[j], c2r.at[sub, slot], 5, recv6.at[sub], z_peers[k])

    def arrived(ref, sem):
        remote(ref, ref, 0, sem, x_peer).wait_recv()

    def left(ref, sem):
        remote(ref, ref, sem, recv1.at[0], x_peer).wait_send()

    def rows_of(m, mine, j):
        k, sub = j // SUBS, j % SUBS
        at = first_at[m] if mine else 1 - first_at[m]
        rows = tok[k, :, sub, at] if m == 0 else tok[k, at, sub]
        return rows.reshape(-1, rows.shape[-1])

    def product(m, mine, dst, js, tiles):
        rows = jnp.concatenate([rows_of(m, mine, j) for j in js], axis=0) if len(js) > 1 else rows_of(m, mine, js[0])
        each = rows.shape[0] // len(js)
        for t in tiles:
            columns = slice(t * TILE, (t + 1) * TILE)
            out = jnp.dot(rows, w1[m, :, columns], preferred_element_type=jnp.float32).astype(jnp.bfloat16)
            for i, j in enumerate(js):
                dst[j, m, :, :, columns] = out[i * each:(i + 1) * each].reshape(2, each // 2, TILE)

    def f32(v):
        return v.astype(jnp.float32)

    def do_s1(j):
        for m in range(2):
            copy_s1(m, j).start()

    def do_s2(j):
        arrived(r1.at[j], recv1.at[j])
        for m in range(2):
            at = 1 - second_at[m]
            s2[j, m] = (f32(own[j, m, at]) + f32(r1[j, m, at])).astype(jnp.bfloat16)
            copy_s2(m, j).start()

    def do_g1(j):
        arrived(r2.at[j], recv2.at[j])
        for m in range(2):
            at = second_at[m]
            pre = f32(own[j, m, at]) + f32(r1[j, m, at]) + f32(r2[j, m])
            hid[j, m, first_at[m], at] = activate(pre[:, :half], pre[:, half:])
            copy_g1(m, j).start()

    def do_g2(j):
        arrived(hid.at[j, :, 0, 0], recv3.at[j])
        for m in range(2):
            copy_g2(m, j).start()

    def do_c1(j):
        arrived(hid.at[j, :, 0], recv4.at[j])
        rows = jnp.concatenate([
            jnp.concatenate([hid[j, 0, b, a], hid[j, 1, a, b]], axis=1)
            for a in (1 - core, core) for b in range(2)
        ], axis=0)
        mid = rows.shape[0] // 2
        for t in range(wd.shape[1] // TILE):
            columns = slice(t * TILE, (t + 1) * TILE)
            out = jnp.dot(rows, wd[:, columns], preferred_element_type=jnp.float32)
            c1s[j, :, columns] = out[:mid].astype(jnp.bfloat16)
            part[j, :, columns] = out[mid:]
        copy_c1(j).start()

    def do_c2(j):
        if j < remote_chunks:
            copy_c1(j).wait_recv()
            c2s[j] = (part[j] + f32(c1r[j])).astype(jnp.bfloat16)
            copy_c2(j).start()
        else:
            sub = j % SUBS
            arrived(c2r.at[sub], recv6.at[sub])
            total = part[j]
            for slot in range(n_z - 1):
                total = total + f32(c2r[sub, slot])
            copy_c1(j).wait_recv()
            out_ref[sub] = (total + f32(c1r[j])).astype(jnp.bfloat16)

    stages = {"s1": do_s1, "s2": do_s2, "g1": do_g1, "g2": do_g2, "c1": do_c1, "c2": do_c2}
    ahead = min(AHEAD, chunks)
    tiles = range(w1.shape[2] // TILE)
    early, late = [j for j in range(chunks) if j < 1], [j for j in range(chunks) if j >= 1]

    load_tok(0).wait()
    for k in range(2):
        load_w1(1, k).start()
    for k in range(2):
        load_w1(0, k).wait()
    product(0, False, s1, early, tiles)
    pl.semaphore_wait(barrier, len(peers))
    copy_s1(0, 0).start()
    for k in range(1, n_z):
        load_tok(k).start()
    for k in range(2):
        load_w1(1, k).wait()
    load_wd.start()
    product(1, False, s1, early, tiles)
    copy_s1(1, 0).start()
    local(tok_hbm.at[pl.ds(1, n_z - 1)], tok.at[pl.ds(1, n_z - 1)], 1).wait()
    for m in range(2):
        product(m, False, s1, late, tiles)
        for j in range(1, ahead):
            copy_s1(m, j).start()
    for m in range(2):
        product(m, True, own, range(chunks), tiles)
    load_wd.wait()

    for stage, j in schedule(chunks, ahead):
        stages[stage](j)

    for ref, sem in ((s1, 0), (s2, 1), (hid.at[:, :, 0, 0], 2), (hid.at[:, :, 0], 3), (c1s, 4), (c2s, 5)):
        left(ref, sem)


def fused(n_row, tokens, w_gate, w_up, w_down):
    n_tok, depth = tokens.shape
    width, features = w_down.shape
    per_row = n_tok // n_row
    n_z, half = n_row // 2, width // 2
    each = per_row // (2 * SUBS)
    chunks = n_z * SUBS
    bf16, dma = jnp.bfloat16, pltpu.SemaphoreType.DMA
    out = pl.pallas_call(
        functools.partial(kernel, n_row),
        out_shape=pltpu.VMEM((SUBS, 2 * each, features), bf16),
        in_specs=[pl.BlockSpec(memory_space=pl.ANY)] * 4,
        out_specs=pl.BlockSpec(memory_space=pltpu.VMEM),
        scratch_shapes=[
            pltpu.VMEM((n_z, 2, SUBS, 2, each, depth), bf16),
            pltpu.VMEM((2, depth, width), bf16),
            pltpu.VMEM((width, features), bf16),
            pltpu.VMEM((chunks, 2, 2, each, width), bf16),
            pltpu.VMEM((chunks, 2, 2, each, width), bf16),
            pltpu.VMEM((chunks, 2, 2, each, width), bf16),
            pltpu.VMEM((chunks, 2, each, width), bf16),
            pltpu.VMEM((chunks, 2, each, width), bf16),
            pltpu.VMEM((chunks, 2, 2, 2, each, half), bf16),
            pltpu.VMEM((chunks, 2 * each, features), jnp.float32),
            pltpu.VMEM((chunks, 2 * each, features), bf16),
            pltpu.VMEM((chunks, 2 * each, features), bf16),
            pltpu.VMEM((chunks - SUBS, 2 * each, features), bf16),
            pltpu.VMEM((SUBS, n_z - 1, 2 * each, features), bf16),
            dma((7,)), dma((6,)),
            dma((chunks,)), dma((chunks,)), dma((chunks,)), dma((chunks,)), dma((chunks,)), dma((SUBS,)),
        ],
        compiler_params=pltpu.CompilerParams(
            collective_id=0, has_side_effects=True, vmem_limit_bytes=62914560
        ),
    )(tokens.reshape(n_z, 2, SUBS, 2, each, depth), w_gate, w_up, w_down)
    return out.reshape(per_row, features)


def solution(mesh):
    n_row, n_col = mesh.shape["row"], mesh.shape["col"]

    def local(tokens, w_gate, w_up, w_down):
        width, features = w_down.shape
        fits = (
            n_col == 4
            and 4 <= n_row <= 16
            and n_row % 2 == 0
            and tokens.shape[0] % (n_row * 32 * SUBS) == 0
            and tokens.shape[0] <= 1024
            and width % TILE == 0
            and features % TILE == 0
            and tokens.shape[1] * width <= 2 ** 21
            and width * features <= 2 ** 21
        )
        if fits:
            return fused(n_row, tokens, w_gate, w_up, w_down)
        return plain(tokens, w_gate, w_up, w_down)

    in_specs = (P(None, "col"), P("col", "row"), P("col", "row"), P("row", "col"))
    return jax.shard_map(local, mesh=mesh, in_specs=in_specs, out_specs=P("row", "col"), check_vma=False)
```

```python
import functools

import jax
import jax.numpy as jnp
from jax import lax
from jax.experimental import pallas as pl
from jax.experimental.pallas import tpu as pltpu
from jax.sharding import PartitionSpec as P

MESH = pl.DeviceIdType.MESH
TILE = 256
SUBS = 2
AHEAD = 3
FLIGHT = 6


def activate(pre_gate, pre_up):
    return (jax.nn.gelu(pre_gate, approximate=True) * pre_up).astype(jnp.bfloat16)


def plain(tokens, w_gate, w_up, w_down):
    joined = jnp.concatenate([w_gate, w_up], axis=1)
    hidden_width = w_gate.shape[1]
    summed = lax.psum_scatter(
        jnp.dot(tokens, joined, preferred_element_type=jnp.float32).astype(jnp.bfloat16),
        "col",
        scatter_dimension=0,
        tiled=True,
    ).astype(jnp.float32)
    hidden = activate(summed[:, :hidden_width], summed[:, hidden_width:])
    hidden_all = lax.all_gather(hidden, "col", axis=0, tiled=True)
    result = lax.psum_scatter(
        jnp.dot(hidden_all, w_down, preferred_element_type=jnp.float32),
        "row",
        scatter_dimension=0,
        tiled=True,
    )
    return result.astype(jnp.bfloat16)


def schedule(chunks, ahead):
    late = {"s2": 0, "g1": 2, "s1": -ahead, "g2": 4, "c2": 7, "c1": 6}
    order = []
    for k in range(chunks + max(late.values())):
        for stage, lag in late.items():
            j = k - lag
            if 0 <= j < chunks and (stage != "s1" or j >= ahead):
                order.append((stage, j))
    return order


def kernel(
    n_row, tok_hbm, wg_hbm, wu_hbm, wd_hbm, out_ref,
    tok, w1, wd, s1, own, r1, s2, r2, hid, part, c1s, c1r, c2s, c2r,
    load_sem, send_sem, recv1, recv2, recv3, recv4, recv5, recv6, ready,
):
    row, col = lax.axis_index("row"), lax.axis_index("col")
    y, x = col // 2, col % 2
    z, core = row // 2, row % 2
    n_z = n_row // 2
    chunks = s1.shape[0]
    remote_chunks = chunks - SUBS
    half = hid.shape[-1]
    x_peer = (row, 2 * y + 1 - x)
    y_peer = (row, 2 * (1 - y) + x)
    core_peer = (2 * z + 1 - core, col)

    def z_order(k):
        return z if k == n_z - 1 else jnp.where(z > k, k, n_z - 1 - k + z)

    blocks = [z_order(k) for k in range(n_z)]
    below, above = z > 0, z < n_z - 1
    z_peers = [(2 * other + core, col) for other in blocks[:-1]]
    first_peer, second_peer = (x_peer, y_peer), (y_peer, x_peer)
    first_at, second_at = (x, y), (y, x)

    barrier = pltpu.get_barrier_semaphore()
    for peer in (x_peer, y_peer, core_peer):
        pl.semaphore_signal(barrier, inc=1, device_id=peer, device_id_type=MESH)
    z_above, z_below = (row + 2, col), (row - 2, col)
    for there, peer in ((above, z_above), (below, z_below)):
        @pl.when(there)
        def _():
            pl.semaphore_signal(barrier, inc=1, device_id=peer, device_id_type=MESH)

    def enter():
        pl.semaphore_wait(barrier, 3 + jnp.where(above, 1, 0) + jnp.where(below, 1, 0))

    def relay(d):
        for side, (here, there, peer) in enumerate(
            ((z >= d, above, z_above), (z <= n_z - 1 - d, below, z_below))
        ):
            @pl.when(jnp.logical_and(here, there))
            def _():
                pl.semaphore_signal(ready.at[d - 1, side], inc=1, device_id=peer, device_id_type=MESH)

    def relayed(d):
        for side, here in enumerate((z > d, z < n_z - 1 - d)):
            @pl.when(here)
            def _():
                pl.semaphore_wait(ready.at[d - 1, side], 1)

    def local(src, dst, sem):
        return pltpu.make_async_copy(src, dst, load_sem.at[sem])

    n_tiles = w1.shape[2] // TILE

    def load_tok(k):
        return local(tok_hbm.at[blocks[k]], tok.at[k], min(k, 1))

    def load_w1(m, t):
        for k, w_hbm in enumerate((wg_hbm, wu_hbm)):
            low, high = max(t * TILE, k * half), min((t + 1) * TILE, (k + 1) * half)
            if low < high:
                local(
                    w_hbm.at[:, pl.ds(m * half + low - k * half, high - low)],
                    w1.at[m, :, pl.ds(low, high - low)],
                    3 + 2 * t + m,
                ).start()

    def wait_w1(m, t):
        columns = pl.ds(t * TILE, TILE)
        local(wg_hbm.at[:, pl.ds(0, TILE)], w1.at[m, :, columns], 3 + 2 * t + m).wait()

    load_wd = local(wd_hbm, wd, 2)
    order_w1 = [(m, t) for t in range(n_tiles) for m in range(2)]
    load_tok(0).start()
    for m, t in order_w1[:FLIGHT]:
        load_w1(m, t)

    def remote(src, dst, send, recv, peer):
        return pltpu.make_async_remote_copy(
            src_ref=src, dst_ref=dst, send_sem=send_sem.at[send], recv_sem=recv, device_id=peer, device_id_type=MESH)

    def copy_s1(m, j):
        return remote(s1.at[j, m], r1.at[j, m], 0, recv1.at[j], first_peer[m])

    def copy_s2(m, j):
        return remote(s2.at[j, m], r2.at[j, m], 1, recv2.at[j], second_peer[m])

    def copy_g1(m, j):
        ref = hid.at[j, m, first_at[m], second_at[m]]
        return remote(ref, ref, 2, recv3.at[j], second_peer[m])

    def copy_g2(m, j):
        ref = hid.at[j, m, first_at[m]]
        return remote(ref, ref, 3, recv4.at[j], first_peer[m])

    def copy_c1(j):
        return remote(c1s.at[j], c1r.at[j], 4, recv5.at[j], core_peer)

    def copy_c2(j):
        k, sub = j // SUBS, j % SUBS
        slot = z - jnp.where(z > blocks[k], 1, 0)
        return remote(c2s.at[j], c2r.at[sub, slot], 5, recv6.at[sub], z_peers[k])

    def arrived(ref, sem):
        remote(ref, ref, 0, sem, x_peer).wait_recv()

    def left(ref, sem):
        remote(ref, ref, sem, recv1.at[0], x_peer).wait_send()

    def rows_of(m, mine, j):
        k, sub = j // SUBS, j % SUBS
        at = first_at[m] if mine else 1 - first_at[m]
        rows = tok[k, :, sub, at] if m == 0 else tok[k, at, sub]
        return rows.reshape(-1, rows.shape[-1])

    def product(m, mine, dst, js, tiles):
        rows = jnp.concatenate([rows_of(m, mine, j) for j in js], axis=0) if len(js) > 1 else rows_of(m, mine, js[0])
        each = rows.shape[0] // len(js)
        for t in tiles:
            columns = slice(t * TILE, (t + 1) * TILE)
            out = jnp.dot(rows, w1[m, :, columns], preferred_element_type=jnp.float32).astype(jnp.bfloat16)
            for i, j in enumerate(js):
                dst[j, m, :, :, columns] = out[i * each:(i + 1) * each].reshape(2, each // 2, TILE)

    def f32(v):
        return v.astype(jnp.float32)

    def do_s1(j):
        for m in range(2):
            copy_s1(m, j).start()

    def do_s2(j):
        arrived(r1.at[j], recv1.at[j])
        for m in range(2):
            at = 1 - second_at[m]
            s2[j, m] = (f32(own[j, m, at]) + f32(r1[j, m, at])).astype(jnp.bfloat16)
            copy_s2(m, j).start()

    def do_g1(j):
        arrived(r2.at[j], recv2.at[j])
        for m in range(2):
            at = second_at[m]
            pre = f32(own[j, m, at]) + f32(r1[j, m, at]) + f32(r2[j, m])
            hid[j, m, first_at[m], at] = activate(pre[:, :half], pre[:, half:])
            copy_g1(m, j).start()

    def do_g2(j):
        arrived(hid.at[j, :, 0, 0], recv3.at[j])
        for m in range(2):
            copy_g2(m, j).start()

    def do_c1(j):
        arrived(hid.at[j, :, 0], recv4.at[j])
        rows = jnp.concatenate([
            jnp.concatenate([hid[j, 0, b, a], hid[j, 1, a, b]], axis=1)
            for a in (1 - core, core) for b in range(2)
        ], axis=0)
        mid = rows.shape[0] // 2
        for t in range(wd.shape[1] // TILE):
            columns = slice(t * TILE, (t + 1) * TILE)
            out = jnp.dot(rows, wd[:, columns], preferred_element_type=jnp.float32)
            c1s[j, :, columns] = out[:mid].astype(jnp.bfloat16)
            part[j, :, columns] = out[mid:]
        copy_c1(j).start()

    def do_c2(j):
        if j < remote_chunks:
            copy_c1(j).wait_recv()
            c2s[j] = (part[j] + f32(c1r[j])).astype(jnp.bfloat16)
            copy_c2(j).start()
        else:
            sub = j % SUBS
            arrived(c2r.at[sub], recv6.at[sub])
            total = part[j]
            for slot in range(n_z - 1):
                total = total + f32(c2r[sub, slot])
            copy_c1(j).wait_recv()
            out_ref[sub] = (total + f32(c1r[j])).astype(jnp.bfloat16)

    stages = {"s1": do_s1, "s2": do_s2, "g1": do_g1, "g2": do_g2, "c1": do_c1, "c2": do_c2}
    ahead = min(AHEAD, chunks)
    tiles = range(n_tiles)
    early, late = range(SUBS), range(SUBS, chunks)

    def copy_tile(m, t):
        columns = pl.ds(t * TILE, TILE)
        return remote(s1.at[0, m, :, :, columns], r1.at[0, m, :, :, columns], 0, recv1.at[0], first_peer[m])

    load_tok(0).wait()
    for i, (m, t) in enumerate(order_w1):
        wait_w1(m, t)
        if i + FLIGHT < len(order_w1):
            load_w1(*order_w1[i + FLIGHT])
        elif i + FLIGHT == len(order_w1):
            for k in range(1, n_z):
                load_tok(k).start()
        product(m, False, s1, early, [t])
        if i == 0:
            enter()
            relay(1)
        copy_tile(m, t).start()
    load_wd.start()
    for j in range(1, min(ahead, SUBS)):
        do_s1(j)
    local(tok_hbm.at[pl.ds(1, n_z - 1)], tok.at[pl.ds(1, n_z - 1)], 1).wait()
    for m in range(2):
        product(m, False, s1, late, tiles)
        for j in range(SUBS, ahead):
            copy_s1(m, j).start()
    for m in range(2):
        product(m, True, own, range(chunks), tiles)
    for d in range(1, n_z - 1):
        relayed(d)
        if d < n_z - 2:
            relay(d + 1)
    load_wd.wait()

    for stage, j in schedule(chunks, ahead):
        stages[stage](j)

    for ref, sem in ((s1, 0), (s2, 1), (hid.at[:, :, 0, 0], 2), (hid.at[:, :, 0], 3), (c1s, 4), (c2s, 5)):
        left(ref, sem)


def fused(n_row, tokens, w_gate, w_up, w_down):
    n_tok, depth = tokens.shape
    width, features = w_down.shape
    per_row = n_tok // n_row
    n_z, half = n_row // 2, width // 2
    each = per_row // (2 * SUBS)
    chunks = n_z * SUBS
    bf16, dma = jnp.bfloat16, pltpu.SemaphoreType.DMA
    out = pl.pallas_call(
        functools.partial(kernel, n_row),
        out_shape=pltpu.VMEM((SUBS, 2 * each, features), bf16),
        in_specs=[pl.BlockSpec(memory_space=pl.ANY)] * 4,
        out_specs=pl.BlockSpec(memory_space=pltpu.VMEM),
        scratch_shapes=[
            pltpu.VMEM((n_z, 2, SUBS, 2, each, depth), bf16),
            pltpu.VMEM((2, depth, width), bf16),
            pltpu.VMEM((width, features), bf16),
            pltpu.VMEM((chunks, 2, 2, each, width), bf16),
            pltpu.VMEM((chunks, 2, 2, each, width), bf16),
            pltpu.VMEM((chunks, 2, 2, each, width), bf16),
            pltpu.VMEM((chunks, 2, each, width), bf16),
            pltpu.VMEM((chunks, 2, each, width), bf16),
            pltpu.VMEM((chunks, 2, 2, 2, each, half), bf16),
            pltpu.VMEM((chunks, 2 * each, features), jnp.float32),
            pltpu.VMEM((chunks, 2 * each, features), bf16),
            pltpu.VMEM((chunks, 2 * each, features), bf16),
            pltpu.VMEM((chunks - SUBS, 2 * each, features), bf16),
            pltpu.VMEM((SUBS, n_z - 1, 2 * each, features), bf16),
            dma((3 + 2 * (width // TILE),)), dma((6,)),
            dma((chunks,)), dma((chunks,)), dma((chunks,)), dma((chunks,)), dma((chunks,)), dma((SUBS,)),
            pltpu.SemaphoreType.REGULAR((n_z - 2, 2)),
        ],
        compiler_params=pltpu.CompilerParams(
            collective_id=0, has_side_effects=True, vmem_limit_bytes=62914560
        ),
    )(tokens.reshape(n_z, 2, SUBS, 2, each, depth), w_gate, w_up, w_down)
    return out.reshape(per_row, features)


def solution(mesh):
    n_row, n_col = mesh.shape["row"], mesh.shape["col"]

    def local(tokens, w_gate, w_up, w_down):
        width, features = w_down.shape
        fits = (
            n_col == 4
            and 6 <= n_row <= 16
            and n_row % 2 == 0
            and tokens.shape[0] % (n_row * 32 * SUBS) == 0
            and tokens.shape[0] <= 1024
            and width % TILE == 0
            and features % TILE == 0
            and tokens.shape[1] * width <= 2 ** 21
            and width * features <= 2 ** 21
        )
        if fits:
            return fused(n_row, tokens, w_gate, w_up, w_down)
        return plain(tokens, w_gate, w_up, w_down)

    in_specs = (P(None, "col"), P("col", "row"), P("col", "row"), P("row", "col"))
    return jax.shard_map(local, mesh=mesh, in_specs=in_specs, out_specs=P("row", "col"), check_vma=False)
```

```python
import functools

import jax
import jax.numpy as jnp
from jax import lax
from jax.experimental import pallas as pl
from jax.experimental.pallas import tpu as pltpu
from jax.sharding import PartitionSpec as P

MESH = pl.DeviceIdType.MESH
TILE = 256
SUBS = 2
MERGED = (6,)
DIRECT = (6, 7)
AHEAD = 4
FLIGHT = 6


def activate(pre_gate, pre_up):
    return (jax.nn.gelu(pre_gate, approximate=True) * pre_up).astype(jnp.bfloat16)


def plain(tokens, w_gate, w_up, w_down):
    joined = jnp.concatenate([w_gate, w_up], axis=1)
    hidden_width = w_gate.shape[1]
    summed = lax.psum_scatter(
        jnp.dot(tokens, joined, preferred_element_type=jnp.float32).astype(jnp.bfloat16),
        "col",
        scatter_dimension=0,
        tiled=True,
    ).astype(jnp.float32)
    hidden = activate(summed[:, :hidden_width], summed[:, hidden_width:])
    hidden_all = lax.all_gather(hidden, "col", axis=0, tiled=True)
    result = lax.psum_scatter(
        jnp.dot(hidden_all, w_down, preferred_element_type=jnp.float32),
        "row",
        scatter_dimension=0,
        tiled=True,
    )
    return result.astype(jnp.bfloat16)


ORDER = (
    ("s2", 1), ("s2", 0), ("s1", 5), ("s2", 2), ("s2", 3), ("g1", 1), ("g1", 0), ("s1", 4),
    ("s2", 5), ("g1", 2), ("g2", 1), ("g1", 3), ("g2", 0), ("s1", 6), ("g1", 5), ("g2", 2),
    ("c1", 1), ("c2", 1), ("s2", 4), ("g2", 3), ("s1", 7), ("c1", 0), ("s2", 6), ("c2", 0),
    ("c1", 2), ("g1", 4), ("c1", 3), ("g2", 5), ("c2", 2), ("s2", 7), ("g2", 4), ("g1", 6),
    ("c2", 3), ("c1", 5), ("g1", 7), ("c2", 5), ("c1", 4), ("c2", 4), ("c1", 6), ("c2", 7),
    ("c2", 6),
)


def schedule(chunks, ahead):
    return ORDER


def kernel(
    n_row, tok_hbm, wg_hbm, wu_hbm, wd_hbm, out_ref,
    tok, w1, wd, s1, own, r1, s2, r2, hid, part, c1s, c1r, c2s, c2r,
    load_sem, send_sem, recv1, recv2, recv3, recv5, recv6, ready,
):
    row, col = lax.axis_index("row"), lax.axis_index("col")
    y, x = col // 2, col % 2
    z, core = row // 2, row % 2
    n_z = n_row // 2
    chunks = s1.shape[0]
    remote_chunks = chunks - SUBS
    half = hid.shape[-1]
    x_peer = (row, 2 * y + 1 - x)
    y_peer = (row, 2 * (1 - y) + x)
    core_peer = (2 * z + 1 - core, col)
    diagonal = (row, 3 - col)

    def z_order(k):
        if k == n_z - 1:
            return z
        order = jnp.where(z > k, k, n_z - 1 - k + z)
        if n_z == 4:
            order = jnp.where(z == 1, (3, 0, 2)[k], order)
        return order

    blocks = [z_order(k) for k in range(n_z)]
    below, above = z > 0, z < n_z - 1
    z_peers = [(2 * other + core, col) for other in blocks[:-1]]
    first_peer, second_peer = (x_peer, y_peer), (y_peer, x_peer)
    first_at, second_at = (x, y), (y, x)

    barrier = pltpu.get_barrier_semaphore()
    near = (x_peer, y_peer, core_peer) + ((diagonal,) if DIRECT else ())
    for peer in near:
        pl.semaphore_signal(barrier, inc=1, device_id=peer, device_id_type=MESH)
    z_above, z_below = (row + 2, col), (row - 2, col)
    for there, peer in ((above, z_above), (below, z_below)):
        @pl.when(there)
        def _():
            pl.semaphore_signal(barrier, inc=1, device_id=peer, device_id_type=MESH)

    def enter():
        pl.semaphore_wait(barrier, len(near) + jnp.where(above, 1, 0) + jnp.where(below, 1, 0))

    def relay(d):
        for side, (here, there, peer) in enumerate(
            ((z >= d, above, z_above), (z <= n_z - 1 - d, below, z_below))
        ):
            @pl.when(jnp.logical_and(here, there))
            def _():
                pl.semaphore_signal(ready.at[d - 1, side], inc=1, device_id=peer, device_id_type=MESH)

    def relayed(d):
        for side, here in enumerate((z > d, z < n_z - 1 - d)):
            @pl.when(here)
            def _():
                pl.semaphore_wait(ready.at[d - 1, side], 1)

    def local(src, dst, sem):
        return pltpu.make_async_copy(src, dst, load_sem.at[sem])

    n_tiles = w1.shape[2] // TILE

    def load_tok(k):
        return local(tok_hbm.at[blocks[k]], tok.at[k], min(k, 1))

    def load_w1(m, t):
        for k, w_hbm in enumerate((wg_hbm, wu_hbm)):
            low, high = max(t * TILE, k * half), min((t + 1) * TILE, (k + 1) * half)
            if low < high:
                local(
                    w_hbm.at[:, pl.ds(m * half + low - k * half, high - low)],
                    w1.at[m, :, pl.ds(low, high - low)],
                    3 + (2 * t + m) % FLIGHT,
                ).start()

    def wait_w1(m, t):
        columns = pl.ds(t * TILE, TILE)
        local(wg_hbm.at[:, pl.ds(0, TILE)], w1.at[m, :, columns], 3 + (2 * t + m) % FLIGHT).wait()

    load_wd = local(wd_hbm, wd, 2)
    order_w1 = [(m, t) for t in range(n_tiles) for m in range(2)]
    load_tok(0).start()
    for m, t in order_w1[:FLIGHT]:
        load_w1(m, t)

    def remote(src, dst, send, recv, peer):
        return pltpu.make_async_remote_copy(
            src_ref=src, dst_ref=dst, send_sem=send_sem.at[send], recv_sem=recv, device_id=peer, device_id_type=MESH)

    def copy_s1(m, j):
        return remote(s1.at[j, m], r1.at[j, m], 0, recv1.at[j], first_peer[m])

    def copy_s2(m, j):
        return remote(s2.at[j, m], r2.at[j, m], 1, recv2.at[j], second_peer[m])

    def copy_g1(m, j):
        ref = hid.at[j, m, first_at[m], second_at[m]]
        return remote(ref, ref, 2, recv1.at[j], second_peer[m])

    def copy_g2(m, j):
        ref = hid.at[j, m, first_at[m]]
        return remote(ref, ref, 3, recv2.at[j], first_peer[m])

    def copy_gd(m, j, peer):
        ref = hid.at[j, m, first_at[m], second_at[m]]
        return remote(ref, ref, 6, recv3.at[j - remote_chunks], peer)

    def copy_c1(j):
        return remote(c1s.at[j], c1r.at[j], 4, recv5.at[j], core_peer)

    def copy_c2(j):
        k, sub = j // SUBS, j % SUBS
        slot = z - jnp.where(z > blocks[k], 1, 0)
        return remote(c2s.at[j], c2r.at[sub, slot], 5, recv6.at[sub], z_peers[k])

    def arrived(ref, sem):
        remote(ref, ref, 0, sem, x_peer).wait_recv()

    def left(ref, sem):
        remote(ref, ref, sem, recv1.at[0], x_peer).wait_send()

    def rows_of(m, mine, j):
        k, sub = j // SUBS, j % SUBS
        at = first_at[m] if mine else 1 - first_at[m]
        rows = tok[k, :, sub, at] if m == 0 else tok[k, at, sub]
        return rows.reshape(-1, rows.shape[-1])

    def product(m, mine, dst, js, tiles):
        rows = jnp.concatenate([rows_of(m, mine, j) for j in js], axis=0) if len(js) > 1 else rows_of(m, mine, js[0])
        each = rows.shape[0] // len(js)
        for t in tiles:
            columns = slice(t * TILE, (t + 1) * TILE)
            out = jnp.dot(rows, w1[m, :, columns], preferred_element_type=jnp.float32).astype(jnp.bfloat16)
            for i, j in enumerate(js):
                dst[j, m, :, :, columns] = out[i * each:(i + 1) * each].reshape(2, each // 2, TILE)

    def f32(v):
        return v.astype(jnp.float32)

    def do_s1(j):
        for m in range(2):
            copy_s1(m, j).start()

    def do_s2(j):
        arrived(r1.at[j], recv1.at[j])
        for m in range(2):
            at = 1 - second_at[m]
            s2[j, m] = (f32(own[j, m, at]) + f32(r1[j, m, at])).astype(jnp.bfloat16)
            copy_s2(m, j).start()

    def do_g1(j):
        arrived(r2.at[j], recv2.at[j])
        for m in range(2):
            at = second_at[m]
            pre = f32(own[j, m, at]) + f32(r1[j, m, at]) + f32(r2[j, m])
            hid[j, m, first_at[m], at] = activate(pre[:, :half], pre[:, half:])
            if j in DIRECT:
                copy_gd(m, j, x_peer).start()
                copy_gd(m, j, y_peer).start()
            else:
                copy_g1(m, j).start()
        if j in DIRECT:
            for m in range(2):
                copy_gd(m, j, diagonal).start()

    def do_g2(j):
        arrived(hid.at[j, :, 0, 0], recv1.at[j])
        for m in range(2):
            copy_g2(m, j).start()

    def do_c1(j):
        js = (j, j + 1) if j in MERGED else (j,)
        for i in js:
            if i in DIRECT:
                arrived(hid.at[:3, :, 0, 0], recv3.at[i - remote_chunks])
            else:
                arrived(hid.at[i, :, 0], recv2.at[i])
        rows = jnp.concatenate([
            jnp.concatenate([hid[i, 0, b, a], hid[i, 1, a, b]], axis=1)
            for a in (1 - core, core) for i in js for b in range(2)
        ], axis=0)
        mid, each = rows.shape[0] // 2, rows.shape[0] // 2 // len(js)
        for t in range(wd.shape[1] // TILE):
            columns = slice(t * TILE, (t + 1) * TILE)
            out = jnp.dot(rows, wd[:, columns], preferred_element_type=jnp.float32)
            for n, i in enumerate(js):
                c1s[i, :, columns] = out[n * each:(n + 1) * each].astype(jnp.bfloat16)
                part[i, :, columns] = out[mid + n * each:mid + (n + 1) * each]
        for i in js:
            copy_c1(i).start()

    def do_c2(j):
        if j < remote_chunks:
            copy_c1(j).wait_recv()
            c2s[j] = (part[j] + f32(c1r[j])).astype(jnp.bfloat16)
            copy_c2(j).start()
        else:
            sub = j % SUBS
            arrived(c2r.at[sub], recv6.at[sub])
            total = part[j]
            for slot in range(n_z - 1):
                total = total + f32(c2r[sub, slot])
            copy_c1(j).wait_recv()
            out_ref[sub] = (total + f32(c1r[j])).astype(jnp.bfloat16)

    stages = {"s1": do_s1, "s2": do_s2, "g1": do_g1, "g2": do_g2, "c1": do_c1, "c2": do_c2}
    ahead = min(AHEAD, chunks)
    tiles = range(n_tiles)
    early, late = range(SUBS), range(SUBS, chunks)

    def copy_tile(m, t, j):
        columns = pl.ds(t * TILE, TILE)
        return remote(s1.at[j, m, :, :, columns], r1.at[j, m, :, :, columns], 0, recv1.at[j], first_peer[m])

    load_tok(0).wait()
    for i, (m, t) in enumerate(order_w1):
        wait_w1(m, t)
        if i + FLIGHT < len(order_w1):
            load_w1(*order_w1[i + FLIGHT])
        elif i + FLIGHT == len(order_w1):
            for k in range(1, n_z):
                load_tok(k).start()
        product(m, False, s1, early, [t])
        if i == 0:
            enter()
            relay(1)
        for j in early:
            copy_tile(m, t, j).start()
    load_wd.start()
    local(tok_hbm.at[pl.ds(1, n_z - 1)], tok.at[pl.ds(1, n_z - 1)], 1).wait()
    for m in range(2):
        product(m, False, s1, late, tiles)
        for j in range(SUBS, ahead):
            copy_s1(m, j).start()
    for m in range(2):
        product(m, True, own, range(chunks), tiles)
    for d in range(1, n_z - 1):
        relayed(d)
        if d < n_z - 2:
            relay(d + 1)
    load_wd.wait()

    for stage, j in schedule(chunks, ahead):
        stages[stage](j)

    paired = chunks - len(DIRECT)
    waits = [(s1, 0), (s2, 1), (hid.at[:paired, :, 0, 0], 2), (hid.at[:paired, :, 0], 3), (c1s, 4), (c2s, 5)]
    if DIRECT:
        waits.append((hid.at[:3 * len(DIRECT), :, 0, 0], 6))
    for ref, sem in waits:
        left(ref, sem)


def fused(n_row, tokens, w_gate, w_up, w_down):
    n_tok, depth = tokens.shape
    width, features = w_down.shape
    per_row = n_tok // n_row
    n_z, half = n_row // 2, width // 2
    each = per_row // (2 * SUBS)
    chunks = n_z * SUBS
    bf16, dma = jnp.bfloat16, pltpu.SemaphoreType.DMA
    out = pl.pallas_call(
        functools.partial(kernel, n_row),
        out_shape=pltpu.VMEM((SUBS, 2 * each, features), bf16),
        in_specs=[pl.BlockSpec(memory_space=pl.ANY)] * 4,
        out_specs=pl.BlockSpec(memory_space=pltpu.VMEM),
        scratch_shapes=[
            pltpu.VMEM((n_z, 2, SUBS, 2, each, depth), bf16),
            pltpu.VMEM((2, depth, width), bf16),
            pltpu.VMEM((width, features), bf16),
            pltpu.VMEM((chunks, 2, 2, each, width), bf16),
            pltpu.VMEM((chunks, 2, 2, each, width), bf16),
            pltpu.VMEM((chunks, 2, 2, each, width), bf16),
            pltpu.VMEM((chunks, 2, each, width), bf16),
            pltpu.VMEM((chunks, 2, each, width), bf16),
            pltpu.VMEM((chunks, 2, 2, 2, each, half), bf16),
            pltpu.VMEM((chunks, 2 * each, features), jnp.float32),
            pltpu.VMEM((chunks, 2 * each, features), bf16),
            pltpu.VMEM((chunks, 2 * each, features), bf16),
            pltpu.VMEM((chunks - SUBS, 2 * each, features), bf16),
            pltpu.VMEM((SUBS, n_z - 1, 2 * each, features), bf16),
            dma((3 + FLIGHT,)), dma((7,)),
            dma((chunks,)), dma((chunks,)), dma((SUBS,)), dma((chunks,)), dma((SUBS,)),
            pltpu.SemaphoreType.REGULAR((n_z - 2, 2)),
        ],
        compiler_params=pltpu.CompilerParams(
            collective_id=0, has_side_effects=True, vmem_limit_bytes=62914560
        ),
    )(tokens.reshape(n_z, 2, SUBS, 2, each, depth), w_gate, w_up, w_down)
    return out.reshape(per_row, features)


def solution(mesh):
    n_row, n_col = mesh.shape["row"], mesh.shape["col"]

    def local(tokens, w_gate, w_up, w_down):
        width, features = w_down.shape
        fits = (
            n_col == 4
            and 6 <= n_row <= 16
            and n_row % 2 == 0
            and tokens.shape[0] % (n_row * 32 * SUBS) == 0
            and tokens.shape[0] <= 1024
            and width % TILE == 0
            and features % TILE == 0
            and tokens.shape[1] * width <= 2 ** 21
            and width * features <= 2 ** 21
        )
        if fits:
            return fused(n_row, tokens, w_gate, w_up, w_down)
        return plain(tokens, w_gate, w_up, w_down)

    in_specs = (P(None, "col"), P("col", "row"), P("col", "row"), P("row", "col"))
    return jax.shard_map(local, mesh=mesh, in_specs=in_specs, out_specs=P("row", "col"), check_vma=False)
```

```python
import functools

import jax
import jax.numpy as jnp
from jax import lax
from jax.experimental import pallas as pl
from jax.experimental.pallas import tpu as pltpu
from jax.sharding import PartitionSpec as P

MESH = pl.DeviceIdType.MESH
TILE = 256
SUBS = 2
MERGED = (6,)
DIRECT = (6, 7)
AHEAD = 3
FLIGHT = 8


def activate(pre_gate, pre_up):
    return (jax.nn.gelu(pre_gate, approximate=True) * pre_up).astype(jnp.bfloat16)


def plain(tokens, w_gate, w_up, w_down):
    joined = jnp.concatenate([w_gate, w_up], axis=1)
    hidden_width = w_gate.shape[1]
    summed = lax.psum_scatter(
        jnp.dot(tokens, joined, preferred_element_type=jnp.float32).astype(jnp.bfloat16),
        "col",
        scatter_dimension=0,
        tiled=True,
    ).astype(jnp.float32)
    hidden = activate(summed[:, :hidden_width], summed[:, hidden_width:])
    hidden_all = lax.all_gather(hidden, "col", axis=0, tiled=True)
    result = lax.psum_scatter(
        jnp.dot(hidden_all, w_down, preferred_element_type=jnp.float32),
        "row",
        scatter_dimension=0,
        tiled=True,
    )
    return result.astype(jnp.bfloat16)


ORDER = (
    ("s1", 3), ("s2", 1), ("s1", 5), ("s2", 2), ("s2", 0), ("s2", 3), ("g1", 1), ("s1", 4),
    ("g1", 2), ("s2", 5), ("g2", 1), ("g1", 0), ("g2", 2), ("g1", 3), ("s2", 4), ("g1", 5),
    ("s1", 6), ("c1", 1), ("c2", 1), ("g2", 0), ("s1", 7), ("g2", 3), ("c1", 2), ("g1", 4),
    ("c2", 2), ("s2", 6), ("g2", 5), ("c1", 0), ("c2", 0), ("s2", 7), ("c1", 3), ("g2", 4),
    ("g1", 6), ("c2", 3), ("c1", 5), ("g1", 7), ("c2", 5), ("c1", 4), ("c2", 4), ("c1", 6),
    ("c2", 7), ("c2", 6),
)


def schedule(chunks, ahead):
    return ORDER, ORDER


def kernel(
    n_row, tok_hbm, wg_hbm, wu_hbm, wd_hbm, out_ref,
    tok, w1, wd, s1, own, r1, s2, r2, hid, part, acc, c1s, c1r, c2s, c2r,
    load_sem, send_sem, recv1, recv2, recv3, recv5, recv6, ready, ready_diagonal,
):
    row, col = lax.axis_index("row"), lax.axis_index("col")
    y, x = col // 2, col % 2
    z, core = row // 2, row % 2
    n_z = n_row // 2
    chunks = s1.shape[0]
    remote_chunks = chunks - SUBS
    half = hid.shape[-1]
    x_peer = (row, 2 * y + 1 - x)
    y_peer = (row, 2 * (1 - y) + x)
    core_peer = (2 * z + 1 - core, col)

    def z_order(k):
        if k == n_z - 1:
            return z
        order = jnp.where(z > k, k, n_z - 1 - k + z)
        if n_z == 4:
            order = jnp.where(z == 1, (3, 0, 2)[k], order)
        return order

    blocks = [z_order(k) for k in range(n_z)]
    below, above = z > 0, z < n_z - 1
    z_peers = [(2 * other + core, col) for other in blocks[:-1]]
    first_peer, second_peer = (x_peer, y_peer), (y_peer, x_peer)
    first_at, second_at = (x, y), (y, x)

    barrier = pltpu.get_barrier_semaphore()
    near = (x_peer, y_peer, core_peer)
    for peer in near:
        pl.semaphore_signal(barrier, inc=1, device_id=peer, device_id_type=MESH)
    z_above, z_below = (row + 2, col), (row - 2, col)
    for there, peer in ((above, z_above), (below, z_below)):
        @pl.when(there)
        def _():
            pl.semaphore_signal(barrier, inc=1, device_id=peer, device_id_type=MESH)

    def enter():
        pl.semaphore_wait(barrier, len(near) + jnp.where(above, 1, 0) + jnp.where(below, 1, 0))

    def relay(d):
        for side, (here, there, peer) in enumerate(
            ((z >= d, above, z_above), (z <= n_z - 1 - d, below, z_below))
        ):
            @pl.when(jnp.logical_and(here, there))
            def _():
                pl.semaphore_signal(ready.at[d - 1, side], inc=1, device_id=peer, device_id_type=MESH)

    def relayed(d):
        for side, here in enumerate((z > d, z < n_z - 1 - d)):
            @pl.when(here)
            def _():
                pl.semaphore_wait(ready.at[d - 1, side], 1)

    def local(src, dst, sem):
        return pltpu.make_async_copy(src, dst, load_sem.at[sem])

    n_tiles = w1.shape[2] // TILE

    def load_tok(k):
        return local(tok_hbm.at[blocks[k]], tok.at[k], min(k, 1))

    def load_w1(m, t):
        for k, w_hbm in enumerate((wg_hbm, wu_hbm)):
            low, high = max(t * TILE, k * half), min((t + 1) * TILE, (k + 1) * half)
            if low < high:
                local(
                    w_hbm.at[:, pl.ds(m * half + low - k * half, high - low)],
                    w1.at[m, :, pl.ds(low, high - low)],
                    3 + (2 * t + m) % FLIGHT,
                ).start()

    def wait_w1(m, t):
        columns = pl.ds(t * TILE, TILE)
        local(wg_hbm.at[:, pl.ds(0, TILE)], w1.at[m, :, columns], 3 + (2 * t + m) % FLIGHT).wait()

    load_wd = local(wd_hbm, wd, 2)
    order_w1 = [(m, t) for t in range(n_tiles) for m in range(2)]
    load_tok(0).start()
    for m, t in order_w1[:FLIGHT]:
        load_w1(m, t)

    def remote(src, dst, send, recv, peer):
        return pltpu.make_async_remote_copy(
            src_ref=src, dst_ref=dst, send_sem=send_sem.at[send], recv_sem=recv, device_id=peer, device_id_type=MESH)

    def copy_s1(m, j):
        return remote(s1.at[j, m], r1.at[j, m], 0, recv1.at[j], first_peer[m])

    def copy_s2(m, j):
        return remote(s2.at[j, m], r2.at[j, m], 1, recv2.at[j], second_peer[m])

    def copy_g1(m, j):
        ref = hid.at[j, m, first_at[m], second_at[m]]
        return remote(ref, ref, 2, recv1.at[j], second_peer[m])

    def copy_g2(m, j):
        ref = hid.at[j, m, first_at[m]]
        return remote(ref, ref, 3, recv2.at[j], first_peer[m])

    def copy_gd(m, j, peer):
        ref = hid.at[j, m, first_at[m], second_at[m]]
        return remote(ref, ref, 6, recv3.at[2 * (j - remote_chunks) + m], peer)

    def copy_c1(j):
        return remote(c1s.at[j], c1r.at[j], 4, recv5.at[j], core_peer)

    def copy_c2(j):
        k, sub = j // SUBS, j % SUBS
        slot = z - jnp.where(z > blocks[k], 1, 0)
        return remote(c2s.at[j], c2r.at[sub, slot], 5, recv6.at[sub], z_peers[k])

    def arrived(ref, sem):
        remote(ref, ref, 0, sem, x_peer).wait_recv()

    def left(ref, sem):
        remote(ref, ref, sem, recv1.at[0], x_peer).wait_send()

    def rows_of(m, mine, j):
        k, sub = j // SUBS, j % SUBS
        at = first_at[m] if mine else 1 - first_at[m]
        rows = tok[k, :, sub, at] if m == 0 else tok[k, at, sub]
        return rows.reshape(-1, rows.shape[-1])

    def product(m, mine, dst, js, tiles):
        rows = jnp.concatenate([rows_of(m, mine, j) for j in js], axis=0) if len(js) > 1 else rows_of(m, mine, js[0])
        each = rows.shape[0] // len(js)
        for t in tiles:
            columns = slice(t * TILE, (t + 1) * TILE)
            out = jnp.dot(rows, w1[m, :, columns], preferred_element_type=jnp.float32).astype(jnp.bfloat16)
            for i, j in enumerate(js):
                dst[j, m, :, :, columns] = out[i * each:(i + 1) * each].reshape(2, each // 2, TILE)

    def f32(v):
        return v.astype(jnp.float32)

    def do_s1(j):
        for m in range(2):
            copy_s1(m, j).start()

    def do_s2(j):
        arrived(r1.at[j], recv1.at[j])
        for m in range(2):
            at = 1 - second_at[m]
            s2[j, m] = (f32(own[j, m, at]) + f32(r1[j, m, at])).astype(jnp.bfloat16)
            copy_s2(m, j).start()

    def do_g1(j):
        arrived(r2.at[j], recv2.at[j])
        for m in range(2):
            at = second_at[m]
            pre = f32(own[j, m, at]) + f32(r1[j, m, at]) + f32(r2[j, m])
            hid[j, m, first_at[m], at] = activate(pre[:, :half], pre[:, half:])
            if j not in DIRECT:
                copy_g1(m, j).start()
        if j in DIRECT:
            for k in range(3):
                for m in range(2):
                    copy_gd(m, j, (row, k + jnp.where(k >= col, 1, 0))).start()

    def do_g2(j):
        arrived(hid.at[j, :, 0, 0], recv1.at[j])
        for m in range(2):
            copy_g2(m, j).start()

    def hidden_rows(m, js):
        return jnp.concatenate([
            hid[j, 0, b, a] if m == 0 else hid[j, 1, a, b]
            for a in (1 - core, core) for j in js for b in range(2)
        ], axis=0)

    def do_c1(j):
        if j in DIRECT:
            do_own(range(j, chunks))
            return
        arrived(hid.at[j, :, 0], recv2.at[j])
        rows = jnp.concatenate([hidden_rows(m, [j]) for m in range(2)], axis=1)
        mid = rows.shape[0] // 2
        for t in range(wd.shape[1] // TILE):
            columns = slice(t * TILE, (t + 1) * TILE)
            out = jnp.dot(rows, wd[:, columns], preferred_element_type=jnp.float32)
            c1s[j, :, columns] = out[:mid].astype(jnp.bfloat16)
            part[j, :, columns] = out[mid:]
        copy_c1(j).start()

    def do_own(js):
        for m in range(2):
            for j in js:
                arrived(hid.at[:3, 0, 0, 0], recv3.at[2 * (j - remote_chunks) + m])
            rows = hidden_rows(m, js)
            mid, each = rows.shape[0] // 2, rows.shape[0] // 2 // len(js)
            for t in range(wd.shape[1] // TILE):
                columns = slice(t * TILE, (t + 1) * TILE)
                out = jnp.dot(rows, wd[m * half:(m + 1) * half, columns], preferred_element_type=jnp.float32)
                if m == 0:
                    acc[:, columns] = out
                    continue
                out = out + acc[:, columns]
                for n, j in enumerate(js):
                    c1s[j, :, columns] = out[n * each:(n + 1) * each].astype(jnp.bfloat16)
                    part[j, :, columns] = out[mid + n * each:mid + (n + 1) * each]
        for j in js:
            copy_c1(j).start()

    def do_c2(j):
        if j < remote_chunks:
            copy_c1(j).wait_recv()
            c2s[j] = (part[j] + f32(c1r[j])).astype(jnp.bfloat16)
            copy_c2(j).start()
        else:
            sub = j % SUBS
            arrived(c2r.at[sub], recv6.at[sub])
            total = part[j]
            for slot in range(n_z - 1):
                total = total + f32(c2r[sub, slot])
            copy_c1(j).wait_recv()
            out_ref[sub] = (total + f32(c1r[j])).astype(jnp.bfloat16)

    stages = {"s1": do_s1, "s2": do_s2, "g1": do_g1, "g2": do_g2, "c1": do_c1, "c2": do_c2}
    ahead = min(AHEAD, chunks)
    tiles = range(n_tiles)
    early, late = range(SUBS), range(SUBS, chunks)

    def copy_tile(m, t, j):
        columns = pl.ds(t * TILE, TILE)
        return remote(s1.at[j, m, :, :, columns], r1.at[j, m, :, :, columns], 0, recv1.at[j], first_peer[m])

    load_tok(0).wait()
    for i, (m, t) in enumerate(order_w1):
        wait_w1(m, t)
        if i + FLIGHT < len(order_w1):
            load_w1(*order_w1[i + FLIGHT])
        elif i + FLIGHT == len(order_w1):
            for k in range(1, n_z):
                load_tok(k).start()
        product(m, False, s1, early, [t])
        if i == 0:
            enter()
            relay(1)
            pl.semaphore_signal(ready_diagonal, inc=1, device_id=x_peer, device_id_type=MESH)
        for j in early:
            copy_tile(m, t, j).start()
    load_wd.start()
    local(tok_hbm.at[pl.ds(1, n_z - 1)], tok.at[pl.ds(1, n_z - 1)], 1).wait()
    for m in range(2):
        product(m, False, s1, late, tiles)
        for j in range(SUBS, ahead):
            copy_s1(m, j).start()
    for m in range(2):
        product(m, True, own, range(chunks), tiles)
    for d in range(1, n_z - 2):
        relayed(d)
        relay(d + 1)
    def run(order):
        known = set()
        for stage, j in order:
            if stage == "c1" and stage not in known:
                load_wd.wait()
                relayed(n_z - 2)
            if stage == "g1" and j in DIRECT and "diagonal" not in known:
                known.add("diagonal")
                pl.semaphore_wait(ready_diagonal, 1)
            known.add(stage)
            stages[stage](j)

    orders = schedule(chunks, ahead)
    if orders[0] == orders[1]:
        run(orders[0])
    else:
        for c in range(2):
            pl.when(core == c)(functools.partial(run, orders[c]))

    if not DIRECT:
        pl.semaphore_wait(ready_diagonal, 1)
    paired = chunks - len(DIRECT)
    waits = [(s1, 0), (s2, 1), (hid.at[:paired, :, 0, 0], 2), (hid.at[:paired, :, 0], 3), (c1s, 4), (c2s, 5)]
    if DIRECT:
        waits.append((hid.at[:3 * len(DIRECT), :, 0, 0], 6))
    for ref, sem in waits:
        left(ref, sem)


def fused(n_row, tokens, w_gate, w_up, w_down):
    n_tok, depth = tokens.shape
    width, features = w_down.shape
    per_row = n_tok // n_row
    n_z, half = n_row // 2, width // 2
    each = per_row // (2 * SUBS)
    chunks = n_z * SUBS
    bf16, dma = jnp.bfloat16, pltpu.SemaphoreType.DMA
    out = pl.pallas_call(
        functools.partial(kernel, n_row),
        out_shape=pltpu.VMEM((SUBS, 2 * each, features), bf16),
        in_specs=[pl.BlockSpec(memory_space=pl.ANY)] * 4,
        out_specs=pl.BlockSpec(memory_space=pltpu.VMEM),
        scratch_shapes=[
            pltpu.VMEM((n_z, 2, SUBS, 2, each, depth), bf16),
            pltpu.VMEM((2, depth, width), bf16),
            pltpu.VMEM((width, features), bf16),
            pltpu.VMEM((chunks, 2, 2, each, width), bf16),
            pltpu.VMEM((chunks, 2, 2, each, width), bf16),
            pltpu.VMEM((chunks, 2, 2, each, width), bf16),
            pltpu.VMEM((chunks, 2, each, width), bf16),
            pltpu.VMEM((chunks, 2, each, width), bf16),
            pltpu.VMEM((chunks, 2, 2, 2, each, half), bf16),
            pltpu.VMEM((chunks, 2 * each, features), jnp.float32),
            pltpu.VMEM((4 * SUBS * each, features), jnp.float32),
            pltpu.VMEM((chunks, 2 * each, features), bf16),
            pltpu.VMEM((chunks, 2 * each, features), bf16),
            pltpu.VMEM((chunks - SUBS, 2 * each, features), bf16),
            pltpu.VMEM((SUBS, n_z - 1, 2 * each, features), bf16),
            dma((3 + FLIGHT,)), dma((7,)),
            dma((chunks,)), dma((chunks,)), dma((2 * SUBS,)), dma((chunks,)), dma((SUBS,)),
            pltpu.SemaphoreType.REGULAR((n_z - 2, 2)),
            pltpu.SemaphoreType.REGULAR,
        ],
        compiler_params=pltpu.CompilerParams(
            collective_id=0, has_side_effects=True, vmem_limit_bytes=62914560
        ),
    )(tokens.reshape(n_z, 2, SUBS, 2, each, depth), w_gate, w_up, w_down)
    return out.reshape(per_row, features)


def solution(mesh):
    n_row, n_col = mesh.shape["row"], mesh.shape["col"]

    def local(tokens, w_gate, w_up, w_down):
        width, features = w_down.shape
        fits = (
            n_col == 4
            and 6 <= n_row <= 16
            and n_row % 2 == 0
            and tokens.shape[0] % (n_row * 32 * SUBS) == 0
            and tokens.shape[0] <= 1024
            and width % TILE == 0
            and features % TILE == 0
            and tokens.shape[1] * width <= 2 ** 21
            and width * features <= 2 ** 21
        )
        if fits:
            return fused(n_row, tokens, w_gate, w_up, w_down)
        return plain(tokens, w_gate, w_up, w_down)

    in_specs = (P(None, "col"), P("col", "row"), P("col", "row"), P("row", "col"))
    return jax.shard_map(local, mesh=mesh, in_specs=in_specs, out_specs=P("row", "col"), check_vma=False)
```

```python
import functools

import jax
import jax.numpy as jnp
from jax import lax
from jax.experimental import pallas as pl
from jax.experimental.pallas import tpu as pltpu
from jax.sharding import PartitionSpec as P

MESH = pl.DeviceIdType.MESH
TILE = 256
SUBS = 2
DIRECT = (6, 7)
AHEAD = 3
FLIGHT = 6


def activate(pre_gate, pre_up):
    return (jax.nn.gelu(pre_gate, approximate=True) * pre_up).astype(jnp.bfloat16)


def plain(tokens, w_gate, w_up, w_down):
    joined = jnp.concatenate([w_gate, w_up], axis=1)
    hidden_width = w_gate.shape[1]
    summed = lax.psum_scatter(
        jnp.dot(tokens, joined, preferred_element_type=jnp.float32).astype(jnp.bfloat16),
        "col",
        scatter_dimension=0,
        tiled=True,
    ).astype(jnp.float32)
    hidden = activate(summed[:, :hidden_width], summed[:, hidden_width:])
    hidden_all = lax.all_gather(hidden, "col", axis=0, tiled=True)
    result = lax.psum_scatter(
        jnp.dot(hidden_all, w_down, preferred_element_type=jnp.float32),
        "row",
        scatter_dimension=0,
        tiled=True,
    )
    return result.astype(jnp.bfloat16)


ORDER = (
    ("s1", 3), ("s2", 0), ("s2", 1), ("s1", 5), ("s2", 3), ("g1", 0), ("s2", 2), ("s1", 4),
    ("g1", 1), ("s2", 5), ("g2", 0), ("g1", 2), ("g1", 3), ("g2", 1), ("s1", 6), ("s2", 4),
    ("c1", 0), ("c2", 0), ("g2", 2), ("g1", 5), ("s1", 7), ("c1", 1), ("c2", 1), ("g2", 3),
    ("g1", 4), ("s2", 6), ("c1", 2), ("g2", 5), ("c2", 2), ("s2", 7), ("c1", 3), ("g2", 4),
    ("c2", 3), ("g1", 6), ("c1", 5), ("g1", 7), ("c2", 5), ("c1", 4), ("c2", 4), ("c1", 6),
    ("c1", 7), ("c2", 7), ("c2", 6),
)


def kernel(
    n_row, tok_hbm, wg_hbm, wu_hbm, wd_hbm, out_ref,
    tok, w1, wd, s1, own, r1, s2, r2, hid, part, acc, c1s, c1r, c2s, c2r,
    load_sem, send_sem, recv1, recv2, recv3, recv5, recv6, ready, ready_diagonal,
):
    row, col = lax.axis_index("row"), lax.axis_index("col")
    y, x = col // 2, col % 2
    z, core = row // 2, row % 2
    n_z = n_row // 2
    chunks = s1.shape[0]
    remote_chunks = chunks - SUBS
    half = hid.shape[-1]
    x_peer = (row, 2 * y + 1 - x)
    y_peer = (row, 2 * (1 - y) + x)
    core_peer = (2 * z + 1 - core, col)

    def z_order(k):
        if k == n_z - 1:
            return z
        order = jnp.where(z > k, k, n_z - 1 - k + z)
        if n_z == 4:
            order = jnp.where(z == 1, (3, 0, 2)[k], order)
        return order

    blocks = [z_order(k) for k in range(n_z)]
    below, above = z > 0, z < n_z - 1
    z_peers = [(2 * other + core, col) for other in blocks[:-1]]
    first_peer, second_peer = (x_peer, y_peer), (y_peer, x_peer)
    first_at, second_at = (x, y), (y, x)

    barrier = pltpu.get_barrier_semaphore()
    near = (x_peer, y_peer, core_peer)
    for peer in near:
        pl.semaphore_signal(barrier, inc=1, device_id=peer, device_id_type=MESH)
    z_above, z_below = (row + 2, col), (row - 2, col)
    for there, peer in ((above, z_above), (below, z_below)):
        @pl.when(there)
        def _():
            pl.semaphore_signal(barrier, inc=1, device_id=peer, device_id_type=MESH)

    def enter():
        pl.semaphore_wait(barrier, len(near) + jnp.where(above, 1, 0) + jnp.where(below, 1, 0))

    def relay(d):
        for side, (here, there, peer) in enumerate(
            ((z >= d, above, z_above), (z <= n_z - 1 - d, below, z_below))
        ):
            @pl.when(jnp.logical_and(here, there))
            def _():
                pl.semaphore_signal(ready.at[d - 1, side], inc=1, device_id=peer, device_id_type=MESH)

    def relayed(d):
        for side, here in enumerate((z > d, z < n_z - 1 - d)):
            @pl.when(here)
            def _():
                pl.semaphore_wait(ready.at[d - 1, side], 1)

    def local(src, dst, sem):
        return pltpu.make_async_copy(src, dst, load_sem.at[sem])

    n_tiles = w1.shape[2] // TILE

    def load_tok(k):
        return local(tok_hbm.at[blocks[k]], tok.at[k], min(k, 1))

    def load_w1(m, t):
        for k, w_hbm in enumerate((wg_hbm, wu_hbm)):
            low, high = max(t * TILE, k * half), min((t + 1) * TILE, (k + 1) * half)
            if low < high:
                local(
                    w_hbm.at[:, pl.ds(m * half + low - k * half, high - low)],
                    w1.at[m, :, pl.ds(low, high - low)],
                    3 + (2 * t + m) % FLIGHT,
                ).start()

    def wait_w1(m, t):
        columns = pl.ds(t * TILE, TILE)
        local(wg_hbm.at[:, pl.ds(0, TILE)], w1.at[m, :, columns], 3 + (2 * t + m) % FLIGHT).wait()

    load_wd = local(wd_hbm, wd, 2)
    order_w1 = [(m, t) for t in range(n_tiles) for m in range(2)]
    load_tok(0).start()
    for m, t in order_w1[:FLIGHT]:
        load_w1(m, t)

    def remote(src, dst, send, recv, peer):
        return pltpu.make_async_remote_copy(
            src_ref=src, dst_ref=dst, send_sem=send_sem.at[send], recv_sem=recv, device_id=peer, device_id_type=MESH)

    def copy_s1(m, j):
        return remote(s1.at[j, m], r1.at[j, m], 0, recv1.at[j], first_peer[m])

    def copy_s2(m, j):
        return remote(s2.at[j, m], r2.at[j, m], 1, recv2.at[j], second_peer[m])

    def copy_g1(m, j):
        ref = hid.at[j, m, first_at[m], second_at[m]]
        return remote(ref, ref, 2, recv1.at[j], second_peer[m])

    def copy_g2(m, j):
        ref = hid.at[j, m, first_at[m]]
        return remote(ref, ref, 3, recv2.at[j], first_peer[m])

    def copy_gd(m, j, peer):
        ref = hid.at[j, m, first_at[m], second_at[m]]
        return remote(ref, ref, 6, recv3.at[2 * (j - remote_chunks) + m], peer)

    def copy_c1(j):
        return remote(c1s.at[j], c1r.at[j], 4, recv5.at[j], core_peer)

    def copy_c2(j):
        k, sub = j // SUBS, j % SUBS
        slot = z - jnp.where(z > blocks[k], 1, 0)
        return remote(c2s.at[j], c2r.at[sub, slot], 5, recv6.at[sub], z_peers[k])

    def arrived(ref, sem):
        remote(ref, ref, 0, sem, x_peer).wait_recv()

    def left(ref, sem):
        remote(ref, ref, sem, recv1.at[0], x_peer).wait_send()

    def rows_of(m, mine, j):
        k, sub = j // SUBS, j % SUBS
        at = first_at[m] if mine else 1 - first_at[m]
        rows = tok[k, :, sub, at] if m == 0 else tok[k, at, sub]
        return rows.reshape(-1, rows.shape[-1])

    def product(m, mine, dst, js, tiles):
        rows = jnp.concatenate([rows_of(m, mine, j) for j in js], axis=0) if len(js) > 1 else rows_of(m, mine, js[0])
        each = rows.shape[0] // len(js)
        for t in tiles:
            columns = slice(t * TILE, (t + 1) * TILE)
            out = jnp.dot(rows, w1[m, :, columns], preferred_element_type=jnp.float32).astype(jnp.bfloat16)
            for i, j in enumerate(js):
                dst[j, m, :, :, columns] = out[i * each:(i + 1) * each].reshape(2, each // 2, TILE)

    def f32(v):
        return v.astype(jnp.float32)

    def do_s1(j):
        for m in range(2):
            copy_s1(m, j).start()

    def do_s2(j):
        arrived(r1.at[j], recv1.at[j])
        for m in range(2):
            at = 1 - second_at[m]
            s2[j, m] = (f32(own[j, m, at]) + f32(r1[j, m, at])).astype(jnp.bfloat16)
            copy_s2(m, j).start()

    def do_g1(j):
        arrived(r2.at[j], recv2.at[j])
        for m in range(2):
            at = second_at[m]
            pre = f32(own[j, m, at]) + f32(r1[j, m, at]) + f32(r2[j, m])
            hid[j, m, first_at[m], at] = activate(pre[:, :half], pre[:, half:])
            if j not in DIRECT:
                copy_g1(m, j).start()
        if j in DIRECT:
            for k in range(3):
                for m in range(2):
                    copy_gd(m, j, (row, k + jnp.where(k >= col, 1, 0))).start()

    def do_g2(j):
        arrived(hid.at[j, :, 0, 0], recv1.at[j])
        for m in range(2):
            copy_g2(m, j).start()

    def hidden_rows(m, js):
        return jnp.concatenate([
            hid[j, 0, b, a] if m == 0 else hid[j, 1, a, b]
            for a in (1 - core, core) for j in js for b in range(2)
        ], axis=0)

    def do_c1(j):
        if j in DIRECT:
            do_own([j])
            return
        arrived(hid.at[j, :, 0], recv2.at[j])
        rows = jnp.concatenate([hidden_rows(m, [j]) for m in range(2)], axis=1)
        mid = rows.shape[0] // 2
        for t in range(wd.shape[1] // TILE):
            columns = slice(t * TILE, (t + 1) * TILE)
            out = jnp.dot(rows, wd[:, columns], preferred_element_type=jnp.float32)
            c1s[j, :, columns] = out[:mid].astype(jnp.bfloat16)
            part[j, :, columns] = out[mid:]
        copy_c1(j).start()

    def do_own(js):
        for m in range(2):
            for j in js:
                arrived(hid.at[:3, 0, 0, 0], recv3.at[2 * (j - remote_chunks) + m])
            rows = hidden_rows(m, js)
            mid, each = rows.shape[0] // 2, rows.shape[0] // 2 // len(js)
            for t in range(wd.shape[1] // TILE):
                columns = slice(t * TILE, (t + 1) * TILE)
                out = jnp.dot(rows, wd[m * half:(m + 1) * half, columns], preferred_element_type=jnp.float32)
                if m == 0:
                    acc[:, columns] = out
                    continue
                out = out + acc[:, columns]
                for n, j in enumerate(js):
                    c1s[j, :, columns] = out[n * each:(n + 1) * each].astype(jnp.bfloat16)
                    part[j, :, columns] = out[mid + n * each:mid + (n + 1) * each]
        for j in js:
            copy_c1(j).start()

    def do_c2(j):
        if j < remote_chunks:
            copy_c1(j).wait_recv()
            c2s[j] = (part[j] + f32(c1r[j])).astype(jnp.bfloat16)
            copy_c2(j).start()
        else:
            sub = j % SUBS
            arrived(c2r.at[sub], recv6.at[sub])
            total = part[j]
            for slot in range(n_z - 1):
                total = total + f32(c2r[sub, slot])
            copy_c1(j).wait_recv()
            out_ref[sub] = (total + f32(c1r[j])).astype(jnp.bfloat16)

    stages = {"s1": do_s1, "s2": do_s2, "g1": do_g1, "g2": do_g2, "c1": do_c1, "c2": do_c2}
    ahead = min(AHEAD, chunks)
    tiles = range(n_tiles)
    early, late = range(SUBS), range(SUBS, chunks)

    def copy_tile(m, t, j):
        columns = pl.ds(t * TILE, TILE)
        return remote(s1.at[j, m, :, :, columns], r1.at[j, m, :, :, columns], 0, recv1.at[j], first_peer[m])

    load_tok(0).wait()
    for i, (m, t) in enumerate(order_w1):
        wait_w1(m, t)
        if i + FLIGHT < len(order_w1):
            load_w1(*order_w1[i + FLIGHT])
        elif i + FLIGHT == len(order_w1):
            for k in range(1, n_z):
                load_tok(k).start()
        product(m, False, s1, early, [t])
        if i == 0:
            enter()
            relay(1)
            pl.semaphore_signal(ready_diagonal, inc=1, device_id=x_peer, device_id_type=MESH)
        for j in early:
            copy_tile(m, t, j).start()
    load_wd.start()
    local(tok_hbm.at[pl.ds(1, n_z - 1)], tok.at[pl.ds(1, n_z - 1)], 1).wait()
    for m in range(2):
        product(m, False, s1, late, tiles)
        for j in range(SUBS, ahead):
            copy_s1(m, j).start()
    for m in range(2):
        product(m, True, own, range(chunks), tiles)
    for d in range(1, n_z - 2):
        relayed(d)
        relay(d + 1)
    known = set()
    for stage, j in ORDER:
        if stage == "c1" and stage not in known:
            load_wd.wait()
            relayed(n_z - 2)
        if stage == "g1" and j in DIRECT and "diagonal" not in known:
            known.add("diagonal")
            pl.semaphore_wait(ready_diagonal, 1)
        known.add(stage)
        stages[stage](j)

    paired = chunks - len(DIRECT)
    waits = [(s1, 0), (s2, 1), (hid.at[:paired, :, 0, 0], 2), (hid.at[:paired, :, 0], 3), (c1s, 4), (c2s, 5)]
    if DIRECT:
        waits.append((hid.at[:3 * len(DIRECT), :, 0, 0], 6))
    for ref, sem in waits:
        left(ref, sem)


def fused(n_row, tokens, w_gate, w_up, w_down):
    n_tok, depth = tokens.shape
    width, features = w_down.shape
    per_row = n_tok // n_row
    n_z, half = n_row // 2, width // 2
    each = per_row // (2 * SUBS)
    chunks = n_z * SUBS
    bf16, dma = jnp.bfloat16, pltpu.SemaphoreType.DMA
    out = pl.pallas_call(
        functools.partial(kernel, n_row),
        out_shape=pltpu.VMEM((SUBS, 2 * each, features), bf16),
        in_specs=[pl.BlockSpec(memory_space=pl.ANY)] * 4,
        out_specs=pl.BlockSpec(memory_space=pltpu.VMEM),
        scratch_shapes=[
            pltpu.VMEM((n_z, 2, SUBS, 2, each, depth), bf16),
            pltpu.VMEM((2, depth, width), bf16),
            pltpu.VMEM((width, features), bf16),
            pltpu.VMEM((chunks, 2, 2, each, width), bf16),
            pltpu.VMEM((chunks, 2, 2, each, width), bf16),
            pltpu.VMEM((chunks, 2, 2, each, width), bf16),
            pltpu.VMEM((chunks, 2, each, width), bf16),
            pltpu.VMEM((chunks, 2, each, width), bf16),
            pltpu.VMEM((chunks, 2, 2, 2, each, half), bf16),
            pltpu.VMEM((chunks, 2 * each, features), jnp.float32),
            pltpu.VMEM((4 * each, features), jnp.float32),
            pltpu.VMEM((chunks, 2 * each, features), bf16),
            pltpu.VMEM((chunks, 2 * each, features), bf16),
            pltpu.VMEM((chunks - SUBS, 2 * each, features), bf16),
            pltpu.VMEM((SUBS, n_z - 1, 2 * each, features), bf16),
            dma((3 + FLIGHT,)), dma((7,)),
            dma((chunks,)), dma((chunks,)), dma((2 * SUBS,)), dma((chunks,)), dma((SUBS,)),
            pltpu.SemaphoreType.REGULAR((n_z - 2, 2)),
            pltpu.SemaphoreType.REGULAR,
        ],
        compiler_params=pltpu.CompilerParams(
            collective_id=0, has_side_effects=True, vmem_limit_bytes=62914560
        ),
    )(tokens.reshape(n_z, 2, SUBS, 2, each, depth), w_gate, w_up, w_down)
    return out.reshape(per_row, features)


def solution(mesh):
    n_row, n_col = mesh.shape["row"], mesh.shape["col"]

    def local(tokens, w_gate, w_up, w_down):
        width, features = w_down.shape
        fits = (
            n_col == 4
            and n_row // 2 * SUBS == 1 + max(j for _, j in ORDER)
            and n_row % 4 == 0
            and tokens.shape[0] % (n_row * 32 * SUBS) == 0
            and tokens.shape[0] <= 1024
            and width % TILE == 0
            and features % TILE == 0
            and tokens.shape[1] * width <= 2 ** 21
            and width * features <= 2 ** 21
        )
        if fits:
            return fused(n_row, tokens, w_gate, w_up, w_down)
        return plain(tokens, w_gate, w_up, w_down)

    in_specs = (P(None, "col"), P("col", "row"), P("col", "row"), P("row", "col"))
    return jax.shard_map(local, mesh=mesh, in_specs=in_specs, out_specs=P("row", "col"), check_vma=False)
```

```python
import functools

import jax
import jax.numpy as jnp
from jax import lax
from jax.experimental import pallas as pl
from jax.experimental.pallas import tpu as pltpu
from jax.sharding import PartitionSpec as P

MESH = pl.DeviceIdType.MESH
TILE = 256
SUBS = 2
DIRECT = (6, 7)
AHEAD = 3
FLIGHT = 6


def activate(pre_gate, pre_up):
    return (jax.nn.gelu(pre_gate, approximate=True) * pre_up).astype(jnp.bfloat16)


def plain(tokens, w_gate, w_up, w_down):
    joined = jnp.concatenate([w_gate, w_up], axis=1)
    hidden_width = w_gate.shape[1]
    summed = lax.psum_scatter(
        jnp.dot(tokens, joined, preferred_element_type=jnp.float32).astype(jnp.bfloat16),
        "col",
        scatter_dimension=0,
        tiled=True,
    ).astype(jnp.float32)
    hidden = activate(summed[:, :hidden_width], summed[:, hidden_width:])
    hidden_all = lax.all_gather(hidden, "col", axis=0, tiled=True)
    result = lax.psum_scatter(
        jnp.dot(hidden_all, w_down, preferred_element_type=jnp.float32),
        "row",
        scatter_dimension=0,
        tiled=True,
    )
    return result.astype(jnp.bfloat16)


ORDER = (
    ("s1", 3), ("s2", 0), ("s2", 1), ("s1", 5), ("s2", 3), ("g1", 0), ("s2", 2), ("s1", 4),
    ("g1", 1), ("s2", 5), ("g2", 0), ("g1", 2), ("g1", 3), ("g2", 1), ("s1", 6), ("s2", 4),
    ("c1", 0), ("c2", 0), ("g2", 2), ("g1", 5), ("s1", 7), ("c1", 1), ("c2", 1), ("g2", 3),
    ("g1", 4), ("s2", 6), ("c1", 2), ("g2", 5), ("c2", 2), ("s2", 7), ("c1", 3), ("g2", 4),
    ("c2", 3), ("g1", 6), ("c1", 5), ("g1", 7), ("c2", 5), ("c1", 4), ("c2", 4), ("c1", 6),
    ("c1", 7), ("c2", 7), ("c2", 6),
)


def kernel(
    n_row, tok_hbm, wg_hbm, wu_hbm, wd_hbm, out_ref,
    tok, w1, wd, s1, own, r1, s2, r2, hid, part, acc, c1s, c1r, c2s, c2r,
    load_sem, send_sem, recv1, recv2, recv3, recv5, recv6, ready, ready_diagonal,
):
    row, col = lax.axis_index("row"), lax.axis_index("col")
    y, x = col // 2, col % 2
    z, core = row // 2, row % 2
    n_z = n_row // 2
    chunks = s1.shape[0]
    remote_chunks = chunks - SUBS
    half = hid.shape[-1]
    x_peer = (row, 2 * y + 1 - x)
    y_peer = (row, 2 * (1 - y) + x)
    core_peer = (2 * z + 1 - core, col)

    def z_order(k):
        if k == n_z - 1:
            return z
        order = jnp.where(z > k, k, n_z - 1 - k + z)
        if n_z == 4:
            order = jnp.where(z == 1, (3, 0, 2)[k], order)
        return order

    blocks = [z_order(k) for k in range(n_z)]
    below, above = z > 0, z < n_z - 1
    z_peers = [(2 * other + core, col) for other in blocks[:-1]]
    first_peer, second_peer = (x_peer, y_peer), (y_peer, x_peer)
    first_at, second_at = (x, y), (y, x)

    barrier = pltpu.get_barrier_semaphore()
    near = (x_peer, y_peer, core_peer)
    for peer in near:
        pl.semaphore_signal(barrier, inc=1, device_id=peer, device_id_type=MESH)
    z_above, z_below = (row + 2, col), (row - 2, col)
    for there, peer in ((above, z_above), (below, z_below)):
        @pl.when(there)
        def _():
            pl.semaphore_signal(barrier, inc=1, device_id=peer, device_id_type=MESH)

    def enter():
        pl.semaphore_wait(barrier, len(near) + jnp.where(above, 1, 0) + jnp.where(below, 1, 0))

    def relay(d):
        for side, (here, there, peer) in enumerate(
            ((z >= d, above, z_above), (z <= n_z - 1 - d, below, z_below))
        ):
            @pl.when(jnp.logical_and(here, there))
            def _():
                pl.semaphore_signal(ready.at[d - 1, side], inc=1, device_id=peer, device_id_type=MESH)

    def relayed(d):
        for side, here in enumerate((z > d, z < n_z - 1 - d)):
            @pl.when(here)
            def _():
                pl.semaphore_wait(ready.at[d - 1, side], 1)

    def local(src, dst, sem):
        return pltpu.make_async_copy(src, dst, load_sem.at[sem])

    n_tiles = w1.shape[2] // TILE

    def load_tok(k):
        return local(tok_hbm.at[blocks[k]], tok.at[k], min(k, 1))

    def load_w1(m, t):
        for k, w_hbm in enumerate((wg_hbm, wu_hbm)):
            low, high = max(t * TILE, k * half), min((t + 1) * TILE, (k + 1) * half)
            if low < high:
                local(
                    w_hbm.at[:, pl.ds(m * half + low - k * half, high - low)],
                    w1.at[m, :, pl.ds(low, high - low)],
                    2 + (2 * t + m) % FLIGHT,
                ).start()

    def wait_w1(m, t):
        columns = pl.ds(t * TILE, TILE)
        local(wg_hbm.at[:, pl.ds(0, TILE)], w1.at[m, :, columns], 2 + (2 * t + m) % FLIGHT).wait()

    load_wd = local(wd_hbm, wd, 0)
    order_w1 = [(m, t) for t in range(n_tiles) for m in range(2)]
    load_tok(0).start()
    for m, t in order_w1[:FLIGHT]:
        load_w1(m, t)

    def remote(src, dst, send, recv, peer):
        return pltpu.make_async_remote_copy(
            src_ref=src, dst_ref=dst, send_sem=send_sem.at[send], recv_sem=recv, device_id=peer, device_id_type=MESH)

    def copy_s1(m, j):
        return remote(s1.at[j, m], r1.at[j, m], 0, recv1.at[j], first_peer[m])

    def copy_s2(m, j):
        return remote(s2.at[j, m], r2.at[j, m], 0, recv2.at[j], second_peer[m])

    def copy_g1(m, j):
        ref = hid.at[j, m, first_at[m], second_at[m]]
        return remote(ref, ref, 0, recv1.at[j], second_peer[m])

    def copy_g2(m, j):
        ref = hid.at[j, m, first_at[m]]
        return remote(ref, ref, 0, recv2.at[j], first_peer[m])

    def copy_gd(m, j, peer):
        ref = hid.at[j, m, first_at[m], second_at[m]]
        return remote(ref, ref, 0, recv3.at[2 * (j - remote_chunks) + m], peer)

    def copy_c1(j):
        return remote(c1s.at[j], c1r.at[j], 1, recv5.at[j], core_peer)

    def copy_c2(j):
        k, sub = j // SUBS, j % SUBS
        slot = z - jnp.where(z > blocks[k], 1, 0)
        return remote(c2s.at[j], c2r.at[sub, slot], 1, recv6.at[sub], z_peers[k])

    def arrived(ref, sem):
        remote(ref, ref, 0, sem, x_peer).wait_recv()

    def left(ref, sem):
        remote(ref, ref, sem, recv1.at[0], x_peer).wait_send()

    def rows_of(m, mine, j):
        k, sub = j // SUBS, j % SUBS
        at = first_at[m] if mine else 1 - first_at[m]
        rows = tok[k, :, sub, at] if m == 0 else tok[k, at, sub]
        return rows.reshape(-1, rows.shape[-1])

    def product(m, mine, dst, js, tiles):
        rows = jnp.concatenate([rows_of(m, mine, j) for j in js], axis=0) if len(js) > 1 else rows_of(m, mine, js[0])
        each = rows.shape[0] // len(js)
        for t in tiles:
            columns = slice(t * TILE, (t + 1) * TILE)
            out = jnp.dot(rows, w1[m, :, columns], preferred_element_type=jnp.float32).astype(jnp.bfloat16)
            for i, j in enumerate(js):
                dst[j, m, :, :, columns] = out[i * each:(i + 1) * each].reshape(2, each // 2, TILE)

    def f32(v):
        return v.astype(jnp.float32)

    def do_s1(j):
        for m in range(2):
            copy_s1(m, j).start()

    def do_s2(j):
        arrived(r1.at[j], recv1.at[j])
        for m in range(2):
            at = 1 - second_at[m]
            s2[j, m] = (f32(own[j, m, at]) + f32(r1[j, m, at])).astype(jnp.bfloat16)
            copy_s2(m, j).start()

    def do_g1(j):
        arrived(r2.at[j], recv2.at[j])
        for m in range(2):
            at = second_at[m]
            pre = f32(own[j, m, at]) + f32(r1[j, m, at]) + f32(r2[j, m])
            hid[j, m, first_at[m], at] = activate(pre[:, :half], pre[:, half:])
            if j not in DIRECT:
                copy_g1(m, j).start()
        if j in DIRECT:
            for k in range(3):
                for m in range(2):
                    copy_gd(m, j, (row, k + jnp.where(k >= col, 1, 0))).start()

    def do_g2(j):
        arrived(hid.at[j, :, 0, 0], recv1.at[j])
        for m in range(2):
            copy_g2(m, j).start()

    def hidden_rows(m, js):
        return jnp.concatenate([
            hid[j, 0, b, a] if m == 0 else hid[j, 1, a, b]
            for a in (1 - core, core) for j in js for b in range(2)
        ], axis=0)

    def do_c1(j):
        if j in DIRECT:
            do_own([j])
            return
        arrived(hid.at[j, :, 0], recv2.at[j])
        rows = jnp.concatenate([hidden_rows(m, [j]) for m in range(2)], axis=1)
        mid = rows.shape[0] // 2
        for t in range(wd.shape[1] // TILE):
            columns = slice(t * TILE, (t + 1) * TILE)
            out = jnp.dot(rows, wd[:, columns], preferred_element_type=jnp.float32)
            c1s[j, :, columns] = out[:mid].astype(jnp.bfloat16)
            part[j, :, columns] = out[mid:]
        copy_c1(j).start()

    def do_own(js):
        for m in range(2):
            for j in js:
                arrived(hid.at[:3, 0, 0, 0], recv3.at[2 * (j - remote_chunks) + m])
            rows = hidden_rows(m, js)
            mid, each = rows.shape[0] // 2, rows.shape[0] // 2 // len(js)
            for t in range(wd.shape[1] // TILE):
                columns = slice(t * TILE, (t + 1) * TILE)
                out = jnp.dot(rows, wd[m * half:(m + 1) * half, columns], preferred_element_type=jnp.float32)
                if m == 0:
                    acc[:, columns] = out
                    continue
                out = out + acc[:, columns]
                for n, j in enumerate(js):
                    c1s[j, :, columns] = out[n * each:(n + 1) * each].astype(jnp.bfloat16)
                    part[j, :, columns] = out[mid + n * each:mid + (n + 1) * each]
        for j in js:
            copy_c1(j).start()

    def do_c2(j):
        if j < remote_chunks:
            copy_c1(j).wait_recv()
            c2s[j] = (part[j] + f32(c1r[j])).astype(jnp.bfloat16)
            copy_c2(j).start()
        else:
            sub = j % SUBS
            arrived(c2r.at[sub], recv6.at[sub])
            total = part[j]
            for slot in range(n_z - 1):
                total = total + f32(c2r[sub, slot])
            copy_c1(j).wait_recv()
            out_ref[sub] = (total + f32(c1r[j])).astype(jnp.bfloat16)

    stages = {"s1": do_s1, "s2": do_s2, "g1": do_g1, "g2": do_g2, "c1": do_c1, "c2": do_c2}
    ahead = min(AHEAD, chunks)
    tiles = range(n_tiles)
    early, late = range(SUBS), range(SUBS, chunks)

    def copy_tile(m, t, j):
        columns = pl.ds(t * TILE, TILE)
        return remote(s1.at[j, m, :, :, columns], r1.at[j, m, :, :, columns], 0, recv1.at[j], first_peer[m])

    load_tok(0).wait()
    for i, (m, t) in enumerate(order_w1):
        wait_w1(m, t)
        if i + FLIGHT < len(order_w1):
            load_w1(*order_w1[i + FLIGHT])
        elif i + FLIGHT == len(order_w1):
            for k in range(1, n_z):
                load_tok(k).start()
        product(m, False, s1, early, [t])
        if i == 0:
            enter()
            relay(1)
            pl.semaphore_signal(ready_diagonal, inc=1, device_id=x_peer, device_id_type=MESH)
        for j in early:
            copy_tile(m, t, j).start()
    load_wd.start()
    local(tok_hbm.at[pl.ds(1, n_z - 1)], tok.at[pl.ds(1, n_z - 1)], 1).wait()
    for m in range(2):
        product(m, False, s1, late, tiles)
        for j in range(SUBS, ahead):
            copy_s1(m, j).start()
    for m in range(2):
        product(m, True, own, range(chunks), tiles)
    for d in range(1, n_z - 2):
        relayed(d)
        relay(d + 1)
    known = set()
    for stage, j in ORDER:
        if stage == "c1" and stage not in known:
            load_wd.wait()
            relayed(n_z - 2)
        if stage == "g1" and j in DIRECT and "diagonal" not in known:
            known.add("diagonal")
            pl.semaphore_wait(ready_diagonal, 1)
        known.add(stage)
        stages[stage](j)

    each = s2.shape[2]
    pieces = chunks * 12 + (chunks - len(DIRECT)) * 6 + len(DIRECT) * 6
    left(w1.at[:, :pieces * each // 4], 0)
    left(wd.at[:(chunks + remote_chunks) * 2 * each], 1)


def fused(n_row, tokens, w_gate, w_up, w_down):
    n_tok, depth = tokens.shape
    width, features = w_down.shape
    per_row = n_tok // n_row
    n_z, half = n_row // 2, width // 2
    each = per_row // (2 * SUBS)
    chunks = n_z * SUBS
    bf16, dma = jnp.bfloat16, pltpu.SemaphoreType.DMA
    out = pl.pallas_call(
        functools.partial(kernel, n_row),
        out_shape=pltpu.VMEM((SUBS, 2 * each, features), bf16),
        in_specs=[pl.BlockSpec(memory_space=pl.ANY)] * 4,
        out_specs=pl.BlockSpec(memory_space=pltpu.VMEM),
        scratch_shapes=[
            pltpu.VMEM((n_z, 2, SUBS, 2, each, depth), bf16),
            pltpu.VMEM((2, depth, width), bf16),
            pltpu.VMEM((width, features), bf16),
            pltpu.VMEM((chunks, 2, 2, each, width), bf16),
            pltpu.VMEM((chunks, 2, 2, each, width), bf16),
            pltpu.VMEM((chunks, 2, 2, each, width), bf16),
            pltpu.VMEM((chunks, 2, each, width), bf16),
            pltpu.VMEM((chunks, 2, each, width), bf16),
            pltpu.VMEM((chunks, 2, 2, 2, each, half), bf16),
            pltpu.VMEM((chunks, 2 * each, features), jnp.float32),
            pltpu.VMEM((4 * each, features), jnp.float32),
            pltpu.VMEM((chunks, 2 * each, features), bf16),
            pltpu.VMEM((chunks, 2 * each, features), bf16),
            pltpu.VMEM((chunks - SUBS, 2 * each, features), bf16),
            pltpu.VMEM((SUBS, n_z - 1, 2 * each, features), bf16),
            dma((2 + FLIGHT,)), dma((2,)),
            dma((chunks,)), dma((chunks,)), dma((2 * SUBS,)), dma((chunks,)), dma((SUBS,)),
            pltpu.SemaphoreType.REGULAR((n_z - 2, 2)),
            pltpu.SemaphoreType.REGULAR,
        ],
        compiler_params=pltpu.CompilerParams(
            collective_id=0, has_side_effects=True, vmem_limit_bytes=62914560
        ),
    )(tokens.reshape(n_z, 2, SUBS, 2, each, depth), w_gate, w_up, w_down)
    return out.reshape(per_row, features)


def solution(mesh):
    n_row, n_col = mesh.shape["row"], mesh.shape["col"]

    def local(tokens, w_gate, w_up, w_down):
        width, features = w_down.shape
        fits = (
            n_col == 4
            and n_row // 2 * SUBS == 1 + max(j for _, j in ORDER)
            and n_row % 4 == 0
            and tokens.shape[0] % (n_row * 32 * SUBS) == 0
            and tokens.shape[0] <= 1024
            and width % TILE == 0
            and features % TILE == 0
            and tokens.shape[1] * width <= 2 ** 21
            and width * features <= 2 ** 21
        )
        if fits:
            return fused(n_row, tokens, w_gate, w_up, w_down)
        return plain(tokens, w_gate, w_up, w_down)

    in_specs = (P(None, "col"), P("col", "row"), P("col", "row"), P("row", "col"))
    return jax.shard_map(local, mesh=mesh, in_specs=in_specs, out_specs=P("row", "col"), check_vma=False)
```
